32 devices in a mesh: tm: 1, space: 32 (over z, y, x, core).
Axes of the slice: x: 2, y: 2, z: 4, core: 2. Of those that a mesh axis runs over, the one named last changes fastest.
Arguments:
- links: float32 [8, 3, 2, 3, 2, 110592], P('tm', None, None, None, None, 'space'), may hold values from -1 to 1, as said below
Outputs:
- new_links: float32 [8, 3, 2, 3, 2, 110592], P('tm', None, None, None, None, 'space')
- theta: float32 [], replicated
- deficit: float32 [8], P('tm')
The draws below stay inside these ranges and needn't reach their ends.
Inputs may be any that keep to these rules, and one draw needn't show every extreme that they name: `links`: each link's two stored rows are orthonormal complex 3-vectors, the first two rows of a special unitary matrix.
All inputs are finite; a program needn't handle non-finite values.
Results may differ from the reference program's by a relative error of at most 0.00013.
Values sent between devices are 32-bit elements; how exact they have to be, the bound alone decides.
A program may use at most 128 MiB of HBM per device.

```python
import math
import jax
import jax.numpy as jnp
from jax import lax

EXTENT = 48
SLICES = 8


def draw_links(key, part):
    sites = EXTENT ** 3
    subkeys = jax.random.split(key, 1)
    site_index = jnp.arange(sites, dtype=jnp.int32)
    row_index = (site_index // EXTENT - 1) % (EXTENT * EXTENT)
    ycoord = (row_index // EXTENT).astype(jnp.float32)
    tcoord = jnp.arange(SLICES, dtype=jnp.float32)
    strength = 0.15 + 0.35 * (0.5 * tcoord[:, None] / SLICES + 0.5 * ycoord[None, :] / EXTENT)
    full_shape = (SLICES, 3, 2, 3, 2, sites)
    noise_field = jnp.clip(0.6 * jax.random.normal(subkeys[0], full_shape, jnp.float32), -1.0, 1.0)
    unit_rows = (jnp.arange(2)[:, None] == jnp.arange(3)[None, :]).astype(jnp.float32)
    unit_rows = unit_rows[:, :, None] * jnp.array([1.0, 0.0], jnp.float32)
    raw_rows = noise_field * strength[:, None, None, None, None, :] + unit_rows[None, None, :, :, :, None]
    vector_one = raw_rows[:, :, 0]
    vector_two = raw_rows[:, :, 1]
    length = jnp.sqrt(jnp.sum(vector_one * vector_one, axis=(2, 3)))
    row_one = vector_one / length[:, :, None, None, :]
    correlation_real = jnp.sum(row_one[:, :, :, 0] * vector_two[:, :, :, 0] + row_one[:, :, :, 1] * vector_two[:, :, :, 1], axis=2)
    correlation_imag = jnp.sum(row_one[:, :, :, 0] * vector_two[:, :, :, 1] - row_one[:, :, :, 1] * vector_two[:, :, :, 0], axis=2)
    rest_real = vector_two[:, :, :, 0] - (correlation_real[:, :, None] * row_one[:, :, :, 0] - correlation_imag[:, :, None] * row_one[:, :, :, 1])
    rest_imag = vector_two[:, :, :, 1] - (correlation_real[:, :, None] * row_one[:, :, :, 1] + correlation_imag[:, :, None] * row_one[:, :, :, 0])
    row_two = jnp.stack([rest_real, rest_imag], axis=3)
    length = jnp.sqrt(jnp.sum(row_two * row_two, axis=(2, 3)))
    row_two = row_two / length[:, :, None, None, :]
    return jnp.stack([row_one, row_two], axis=2).astype(jnp.float32)


def setup_inputs(seed: int = 0) -> dict:
    splits = jax.random.split(jax.random.key(seed), 2)
    links = draw_links(jax.random.fold_in(splits[1], 71), 0)
    return dict(links=links)


root_three = math.sqrt(3.0)
step_size = 0.08
top_momentum = 12.0
storage_offset = 1

def complex_mul(p, q):
    return (p[0] * q[0] - p[1] * q[1], p[0] * q[1] + p[1] * q[0])

def complex_add(p, q):
    return (p[0] + q[0], p[1] + q[1])

def complex_sub(p, q):
    return (p[0] - q[0], p[1] - q[1])

def complex_conj(p):
    return (p[0], -p[1])

def matrix_mul(left, right):
    rows_out = []
    for i in range(len(left)):
        entries = []
        for j in range(3):
            summed = complex_mul(left[i][0], right[0][j])
            for k in (1, 2):
                summed = complex_add(summed, complex_mul(left[i][k], right[k][j]))
            entries.append(summed)
        rows_out.append(entries)
    return rows_out

def dagger_of(matrix):
    return [[complex_conj(matrix[j][i]) for j in range(3)] for i in range(3)]

def cross_conj(row_one, row_two):
    row_three = []
    for k in range(3):
        a = complex_mul(row_one[(k + 1) % 3], row_two[(k + 2) % 3])
        b = complex_mul(row_one[(k + 2) % 3], row_two[(k + 1) % 3])
        row_three.append(complex_conj(complex_sub(a, b)))
    return row_three

def full_matrix(entry_of):
    row_one = [(entry_of(0, c, 0), entry_of(0, c, 1)) for c in range(3)]
    row_two = [(entry_of(1, c, 0), entry_of(1, c, 1)) for c in range(3)]
    return [row_one, row_two, cross_conj(row_one, row_two)]

def gradient_of(current, behind):
    gradient = []
    for i in range(3):
        entries = []
        for j in range(3):
            summed = complex_sub(behind[0][i][j], current[0][i][j])
            for d in (1, 2):
                summed = complex_add(summed, complex_sub(behind[d][i][j], current[d][i][j]))
            entries.append(summed)
        gradient.append(entries)
    return gradient

def algebra_of(gradient):
    g = gradient
    return [g[0][1][1] + g[1][0][1], g[0][1][0] - g[1][0][0], g[0][0][1] - g[1][1][1], g[0][2][1] + g[2][0][1], g[0][2][0] - g[2][0][0], g[1][2][1] + g[2][1][1], g[1][2][0] - g[2][1][0], (g[0][0][1] + g[1][1][1] - 2.0 * g[2][2][1]) / root_three]

def rotation_of(algebra):
    half_step = 0.5 * step_size
    zeros_like = jnp.zeros_like(algebra[0])
    diag_zero = algebra[2] + algebra[7] / root_three
    diag_one = -algebra[2] + algebra[7] / root_three
    diag_two = -2.0 * algebra[7] / root_three
    hermitian = [[(diag_zero, zeros_like), (algebra[0], -algebra[1]), (algebra[3], -algebra[4])], [(algebra[0], algebra[1]), (diag_one, zeros_like), (algebra[5], -algebra[6])], [(algebra[3], algebra[4]), (algebra[5], algebra[6]), (diag_two, zeros_like)]]
    generator = [[(-half_step * h[1], half_step * h[0]) for h in row] for row in hermitian]
    square = matrix_mul(generator[:2], generator)
    rows_two = []
    for i in range(2):
        entries = []
        for j in range(3):
            real_value = generator[i][j][0] + 0.5 * square[i][j][0]
            if i == j:
                real_value = real_value + 1.0
            entries.append((real_value, generator[i][j][1] + 0.5 * square[i][j][1]))
        rows_two.append(entries)
    length = jnp.sqrt(sum((p[0] * p[0] + p[1] * p[1] for p in rows_two[0])))
    row_one = [(p[0] / length, p[1] / length) for p in rows_two[0]]
    correlation = complex_mul(complex_conj(row_one[0]), rows_two[1][0])
    for k in (1, 2):
        correlation = complex_add(correlation, complex_mul(complex_conj(row_one[k]), rows_two[1][k]))
    row_two = [complex_sub(rows_two[1][k], complex_mul(correlation, row_one[k])) for k in range(3)]
    length = jnp.sqrt(sum((p[0] * p[0] + p[1] * p[1] for p in row_two)))
    row_two = [(p[0] / length, p[1] / length) for p in row_two]
    return [row_one, row_two, cross_conj(row_one, row_two)]

def two_rows(product, axis):
    return jnp.stack([jnp.stack([jnp.stack(product[r][c], axis=axis) for c in range(3)], axis=axis) for r in range(2)], axis=axis)

def reference(links):
    extent = EXTENT
    slice_count = links.shape[0]
    wave_number = jnp.arange(extent, dtype=jnp.int32)
    wave_term = 4.0 * jnp.sin(math.pi * wave_number.astype(jnp.float32) / extent) ** 2
    momentum = wave_term[:, None, None] + wave_term[None, :, None] + wave_term[None, None, :]
    zero_mode = wave_number[:, None, None] + wave_number[None, :, None] + wave_number[None, None, :] == 0
    factor = jnp.where(zero_mode, 0.0, top_momentum / jnp.where(zero_mode, 1.0, momentum))
    roll_axes = (-1, -3, -2)

    def one_slice(slice_links):
        ordered = jnp.roll(slice_links, -storage_offset * extent, axis=-1)
        lattice = ordered.reshape(3, 2, 3, 2, extent, extent, extent)
        current = []
        behind = []
        for d in range(3):
            here = lattice[d]
            moved = jnp.roll(here, 1, axis=roll_axes[d])
            current.append(full_matrix(lambda r, c, p, arr=here: arr[r, c, p]))
            behind.append(full_matrix(lambda r, c, p, arr=moved: arr[r, c, p]))
        algebra = algebra_of(gradient_of(current, behind))
        theta_part = sum((jnp.sum(a * a) for a in algebra))
        spectrum = jnp.fft.fftn(jnp.stack(algebra), axes=(1, 2, 3))
        smooth = jnp.real(jnp.fft.ifftn(spectrum * factor, axes=(1, 2, 3))).astype(jnp.float32)
        rotation = rotation_of([smooth[a] for a in range(8)])
        new_dirs = []
        deficit_part = jnp.zeros((), jnp.float32)
        for d in range(3):
            ahead_rot = jax.tree.map(lambda a, ax=roll_axes[d]: jnp.roll(a, -1, axis=ax), rotation)
            product = matrix_mul(matrix_mul(rotation, current[d]), dagger_of(ahead_rot))
            deficit_part = deficit_part + jnp.sum(3.0 - product[0][0][0] - product[1][1][0] - product[2][2][0])
            new_dirs.append(two_rows(product, 0))
        result = jnp.stack(new_dirs).reshape(3, 2, 3, 2, extent ** 3)
        return (jnp.roll(result, storage_offset * extent, axis=-1), theta_part, deficit_part)
    new_links, thetas, deficits = lax.map(one_slice, links)
    theta = jnp.sum(thetas) / (slice_count * extent ** 3)
    deficit = deficits / extent ** 3
    return (new_links, theta, deficit)
```

```python
import functools
import math

import jax
import jax.numpy as jnp
import numpy as np
from jax import lax
from jax.experimental import pallas as pl
from jax.experimental.pallas import tpu as pltpu
from jax.sharding import PartitionSpec as P

EXTENT = 48
LANES = 128
HALF = 64
SEG = 16

root_three = math.sqrt(3.0)
step_size = 0.08
top_momentum = 12.0

f32 = jnp.float32
bf16 = jnp.bfloat16
MESH = pl.DeviceIdType.MESH
VM = pl.BlockSpec(memory_space=pltpu.VMEM)
PARAMS = pltpu.CompilerParams(vmem_limit_bytes=60 * 1024 * 1024)


def from_behind(block, axis, distance):
    n = lax.axis_size(axis)
    return lax.ppermute(block, axis, [((i - distance) % n, i) for i in range(n)])


def cmul(p, q):
    return (p[0] * q[0] - p[1] * q[1], p[0] * q[1] + p[1] * q[0])


def cadd(p, q):
    return (p[0] + q[0], p[1] + q[1])


def csub(p, q):
    return (p[0] - q[0], p[1] - q[1])


def conj(p):
    return (p[0], -p[1])


def conj_mul(p, q):
    return (p[0] * q[0] + p[1] * q[1], p[0] * q[1] - p[1] * q[0])


def mul_conj(p, q):
    return (p[0] * q[0] + p[1] * q[1], p[1] * q[0] - p[0] * q[1])


def dot_row(row, col, mul):
    out = mul(row[0], col[0])
    for k in (1, 2):
        out = cadd(out, mul(row[k], col[k]))
    return out


def cross_conj(a, b):
    return [
        conj(csub(cmul(a[(k + 1) % 3], b[(k + 2) % 3]), cmul(a[(k + 2) % 3], b[(k + 1) % 3])))
        for k in range(3)
    ]


def algebra_of(u):
    return [
        u[0][1][1] + u[1][0][1],
        u[0][1][0] - u[1][0][0],
        u[0][0][1] - u[1][1][1],
        u[0][2][1] + u[2][0][1],
        u[0][2][0] - u[2][0][0],
        u[1][2][1] + u[2][1][1],
        u[1][2][0] - u[2][1][0],
        (u[0][0][1] + u[1][1][1] - 2.0 * u[2][2][1]) * (1.0 / root_three),
    ]


def rotation_of(s):
    h = 0.5 * step_size
    s = [v * h for v in s]
    third = s[7] * (1.0 / root_three)
    d0, d1, d2 = s[2] + third, third - s[2], -2.0 * third
    herm = [
        [(d0, None), (s[0], -s[1]), (s[3], -s[4])],
        [(s[0], s[1]), (d1, None), (s[5], -s[6])],
        [(s[3], s[4]), (s[5], s[6]), (d2, None)],
    ]

    def mul(p, q):
        if p[1] is None and q[1] is None:
            return (p[0] * q[0], jnp.zeros_like(p[0]))
        if p[1] is None:
            return (p[0] * q[0], p[0] * q[1])
        if q[1] is None:
            return (p[0] * q[0], p[1] * q[0])
        return cmul(p, q)

    rows = []
    for i in range(2):
        row = []
        for j in range(3):
            sq = dot_row(herm[i], [herm[k][j] for k in range(3)], mul)
            re, im = -0.5 * sq[0], -0.5 * sq[1]
            if herm[i][j][1] is not None:
                re = re - herm[i][j][1]
            else:
                re = re + 1.0
            row.append((re, im + herm[i][j][0]))
        rows.append(row)

    def unit(row):
        inv = lax.rsqrt(sum(p[0] * p[0] + p[1] * p[1] for p in row))
        return [(p[0] * inv, p[1] * inv) for p in row]

    one = unit(rows[0])
    corr = dot_row(one, rows[1], conj_mul)
    two = unit([csub(rows[1][k], cmul(corr, one[k])) for k in range(3)])
    return [one, two, cross_conj(one, two)]


def block(k):
    return pl.ds(pl.multiple_of(k * LANES, LANES), LANES)


def lane_ids(rows=8):
    return lax.broadcasted_iota(jnp.int32, (rows, LANES), 1)


def load_link(ref, d, sl):
    rows = [[(ref[d, r, c, 0, :, sl], ref[d, r, c, 1, :, sl]) for c in range(3)] for r in range(2)]
    return rows + [cross_conj(rows[0], rows[1])]


def algebra_kernel(links, out):
    def step(k, carry):
        sl = block(k)
        for d in range(3):
            for a, v in enumerate(algebra_of(load_link(links, d, sl))):
                out[d, a, :, sl] = v
        return carry

    lax.fori_loop(0, links.shape[-1] // LANES, step, 0)


def split3(x):
    hi = x.astype(bf16)
    lo = (x - hi.astype(f32)).astype(bf16)
    return jnp.concatenate([hi, lo, hi], axis=0)


def transform(table, parts, sign):
    n = parts[0].shape[0]
    both = jnp.dot(table, split3(jnp.concatenate(parts, axis=1)), preferred_element_type=f32)
    outs = []
    for i in range(len(parts)):
        mine = both[:, i * LANES : (i + 1) * LANES]
        swapped = pltpu.roll(mine[n:], HALF, 1)
        outs.append(mine[:n] + jnp.where(lane_ids(n) < HALF, sign, -sign) * swapped)
    return outs


def spread_kernel(extent, head, nsplit, alg, y_rim, z_below, z_above, coords, table, out, theta, mat, rows, freq):
    nb = alg.shape[-1] // LANES
    yb = y_rim.shape[-1] // LANES
    qh = head // extent
    hb = head // LANES
    lane = lane_ids()
    mat[...] = jnp.zeros_like(mat)

    def step(k, total):
        sl = block(k)
        before = block(jnp.maximum(k - 1, 0))
        after = block(jnp.minimum(k + 1, nb - 1))
        edge_x = coords[0, :, sl] == 0
        edge_z = coords[1, :, sl] == 0
        second = (k >= hb).astype(jnp.int32)
        dst = block(k - second * hb)
        for a in range(8):
            x, y, z = alg[0, a, :, sl], alg[1, a, :, sl], alg[2, a, :, sl]
            near = pltpu.roll(jnp.where(lane == LANES - 1, alg[0, a, :, before], x), 1, 1)
            far = pltpu.roll(jnp.where(lane < extent - 1, alg[0, a, :, after], x), LANES - extent + 1, 1)
            bx = jnp.where(edge_x, far, near)
            by = jnp.where(
                k < yb,
                y_rim[a, :, block(jnp.minimum(k, yb - 1))],
                alg[1, a, :, block(jnp.maximum(k - yb, 0))],
            )
            prev = jnp.where(k == 0, z_below[a], alg[2, a, :, before])
            near = pltpu.roll(jnp.where(lane >= LANES - extent, prev, z), extent, 1)
            far = pltpu.roll(jnp.where(k == 0, alg[2, a, :, block(yb)], z_above[a]), extent, 1)
            bz = jnp.where(edge_z, far, near)
            b = (bx - x) + (by - y) + (bz - z)
            total = total + b * b
            mat[pl.ds(pl.multiple_of((a % 2) * HALF + second * (HALF // 2) + (a // 2) * 8, 8), 8), dst] = b
        return total

    theta[...] = lax.fori_loop(0, nb, step, jnp.zeros((8, LANES), f32))
    for k in range(hb):
        rows[k * LANES : (k + 1) * LANES, :] = mat[:, k * LANES : (k + 1) * LANES].T

    def dft(i, carry):
        parts = [rows[pl.ds(pl.multiple_of((2 * i + e) * extent, 8), extent), :] for e in range(2)]
        for e, v in enumerate(transform(table[...], parts, 1.0)):
            freq[pl.ds(pl.multiple_of((2 * i + e) * extent, 8), extent), :] = v
        return carry

    lax.fori_loop(0, qh // 2, dft, 0, unroll=2)
    count = extent // (out.shape[0] // nsplit)
    q = out.shape[1]
    seg = lax.rem(lane_ids(qh), HALF) // SEG

    def pack(j, carry):
        vals = [freq[pl.ds(j * count + m, qh, stride=extent), :] for m in range(count)]
        for c in range(nsplit):
            for h in range(2):
                acc = jnp.zeros((qh, LANES), f32)
                for m in range(count):
                    moved = pltpu.roll(vals[m], ((m - (2 * h + c)) * SEG) % LANES, 1)
                    acc = jnp.where(seg == m, moved, acc)
                lo, hi = (0, qh) if h == 0 else (qh, q)
                out[j * nsplit + c, lo:hi, :] = acc[: hi - lo]
        return carry

    lax.fori_loop(0, out.shape[0] // nsplit, pack, 0)


def plane_kernel(extent, planes, wave, wave_lane, table, out, one, two):
    n = extent
    total = n * n
    scale = top_momentum / float(n) ** 3
    for y in range(n - 1):
        one[y * n : (y + 1) * n, :] = planes[y * n + 1 : (y + 1) * n + 1, :]
    one[total - n : total - 1, :] = planes[total - n + 1 : total, :]
    one[total - 1 : total, :] = planes[0:1, :]

    def rows_at(i):
        return pl.ds(pl.multiple_of(i * n, 8), n)

    def along_z(i, carry):
        parts = [one[rows_at(2 * i + e), :] for e in range(2)]
        for e, v in enumerate(transform(table[...], parts, 1.0)):
            two[rows_at(2 * i + e), :] = v
        return carry

    lax.fori_loop(0, n // 2, along_z, 0, unroll=2)

    def along_y(i, carry):
        parts = [two[pl.ds(2 * i + e, n, stride=n), :] for e in range(2)]
        vals = transform(table[...], parts, 1.0)
        done = []
        for e, v in enumerate(vals):
            p2 = wave[...] + (wave_lane[...] + wave[pl.ds(2 * i + e, 1), :])
            zero = p2 == 0.0
            done.append(v * jnp.where(zero, 0.0, scale / jnp.where(zero, 1.0, p2)))
        for e, v in enumerate(transform(table[...], done, -1.0)):
            one[rows_at(2 * i + e), :] = v
        return carry

    lax.fori_loop(0, n // 2, along_y, 0, unroll=2)

    def back_z(i, carry):
        parts = [one[pl.ds(2 * i + e, n, stride=n), :] for e in range(2)]
        for e, v in enumerate(transform(table[...], parts, -1.0)):
            two[rows_at(2 * i + e), :] = v
        return carry

    lax.fori_loop(0, n // 2, back_z, 0, unroll=2)
    out[0:1, :] = two[total - 1 : total, :]
    for y in range(n - 1):
        out[y * n + 1 : (y + 1) * n + 1, :] = two[y * n : (y + 1) * n, :]
    out[total - n + 1 : total, :] = two[total - n : total - 1, :]


def gather_kernel(extent, head, nsplit, planes, table, out, mat, rows, freq):
    hb = head // LANES
    qh = head // extent
    nb = out.shape[-1] // LANES
    q = planes.shape[1]
    rest = q - qh
    count = extent // (planes.shape[0] // nsplit)
    seg = lax.rem(lane_ids(rest), HALF) // SEG
    seg_tail = lax.rem(lane_ids(qh - rest), HALF) // SEG

    def unpack(j, carry):
        for m in range(count):
            acc = jnp.zeros((rest, LANES), f32)
            tail = jnp.zeros((qh - rest, LANES), f32)
            for c in range(nsplit):
                for h in range(2):
                    s = 2 * h + c
                    shift = ((s - m) * SEG) % LANES
                    lo = h * qh
                    acc = jnp.where(seg == s, pltpu.roll(planes[j * nsplit + c, lo : lo + rest, :], shift, 1), acc)
                    if h == 0:
                        tail = jnp.where(
                            seg_tail == s, pltpu.roll(planes[j * nsplit + c, rest:qh, :], shift, 1), tail
                        )
            freq[pl.ds(j * count + m, qh, stride=extent), :] = jnp.concatenate([acc, tail], axis=0)
        return carry

    lax.fori_loop(0, planes.shape[0] // nsplit, unpack, 0)

    def dft(i, carry):
        parts = [freq[pl.ds(pl.multiple_of((2 * i + e) * extent, 8), extent), :] for e in range(2)]
        for e, v in enumerate(transform(table[...], parts, -1.0)):
            rows[pl.ds(pl.multiple_of((2 * i + e) * extent, 8), extent), :] = v
        return carry

    lax.fori_loop(0, qh // 2, dft, 0, unroll=2)
    for k in range(hb):
        turned = rows[k * LANES : (k + 1) * LANES, :].T
        for a in range(8):
            first = (a % 2) * HALF + (a // 2) * 8
            out[a, :, k * LANES : (k + 1) * LANES] = turned[first : first + 8]
            if hb + k < nb:
                second = first + HALF // 2
                out[a, :, (hb + k) * LANES : (hb + k + 1) * LANES] = turned[second : second + 8]


def link_kernel(extent, links, smooth, above, below, coords, out, deficit, rot):
    nb = smooth.shape[-1] // LANES
    yb = above.shape[-1] // LANES
    lane = lane_ids()

    def rotate(values, sl):
        g = rotation_of(values)
        for i in range(3):
            for j in range(3):
                for p in range(2):
                    rot[6 * i + 2 * j + p, :, sl] = g[i][j][p]

    def rotate_own(k, carry):
        rotate([smooth[a, :, block(k)] for a in range(8)], block(k))
        return carry

    def rotate_above(k, carry):
        rotate([above[a, :, block(k)] for a in range(8)], block(nb + k))
        return carry

    lax.fori_loop(0, nb, rotate_own, 0)
    lax.fori_loop(0, yb, rotate_above, 0)
    rotate([below[a] for a in range(8)], block(nb + yb))

    def step(k, total):
        sl = block(k)
        before = block(jnp.maximum(k - 1, 0))
        after = block(k + 1)
        wrap = block(jnp.where(k == yb, 0, nb + yb))
        edge_x = coords[0, :, sl] == extent - 1
        edge_z = coords[1, :, sl] == extent - 1

        def ahead_x(e):
            cur = rot[e, :, sl]
            near = pltpu.roll(jnp.where(lane == 0, rot[e, :, after], cur), LANES - 1, 1)
            far = pltpu.roll(jnp.where(lane >= LANES - extent + 1, rot[e, :, before], cur), extent - 1, 1)
            return jnp.where(edge_x, far, near)

        def ahead_y(e):
            return rot[e, :, block(k + yb)]

        def ahead_z(e):
            cur = rot[e, :, sl]
            near = pltpu.roll(jnp.where(lane < extent, rot[e, :, after], cur), LANES - extent, 1)
            far = pltpu.roll(rot[e, :, wrap], LANES - extent, 1)
            return jnp.where(edge_z, far, near)

        for d, ahead in enumerate((ahead_x, ahead_y, ahead_z)):
            u = load_link(links, d, sl)
            own = [[(rot[6 * i + 2 * j, :, sl], rot[6 * i + 2 * j + 1, :, sl]) for j in range(3)] for i in range(3)]
            left = [
                [dot_row(own[i], [u[k2][j] for k2 in range(3)], cmul) for j in range(3)]
                for i in range(3)
            ]
            for j in range(3):
                row = [(ahead(6 * j + 2 * c), ahead(6 * j + 2 * c + 1)) for c in range(3)]
                for i in range(2):
                    v = dot_row(left[i], row, mul_conj)
                    out[d, i, j, 0, :, sl] = v[0]
                    out[d, i, j, 1, :, sl] = v[1]
                    if i == j:
                        total = total + (1.0 - v[0])
                if j == 2:
                    total = total + (1.0 - dot_row(left[2], row, mul_conj)[0])
        return total

    deficit[...] = lax.fori_loop(0, nb, step, jnp.zeros((8, LANES), f32))


def sum_kernel(n, theta, deficit, out, mine, held, send_sem, recv_sem):
    me = lax.axis_index("space")
    barrier = pltpu.get_barrier_semaphore()
    for i in range(1, n):
        pl.semaphore_signal(barrier, inc=1, device_id={"space": lax.rem(me + i, n)}, device_id_type=MESH)
    lane = lane_ids()
    t = jnp.sum(jnp.sum(theta[...], axis=1, keepdims=True), axis=0, keepdims=True)
    d = jnp.sum(deficit[...], axis=1, keepdims=True)
    mine[...] = jnp.where(lane == 0, d, jnp.where(lane == 1, t, 0.0))
    pl.semaphore_wait(barrier, n - 1)
    copies = []
    for i in range(1, n):
        copy = pltpu.make_async_remote_copy(
            src_ref=mine,
            dst_ref=held.at[i],
            send_sem=send_sem.at[i],
            recv_sem=recv_sem.at[i],
            device_id={"space": lax.rem(me + i, n)},
            device_id_type=MESH,
        )
        copy.start()
        copies.append(copy)
    for copy in copies:
        copy.wait()
    total = mine[...]
    for i in range(1, n):
        total = total + held[i]
    out[...] = total


def call(kernel, out_shape, scratch, *args, params=PARAMS):
    return pl.pallas_call(
        kernel,
        out_shape=out_shape,
        in_specs=[VM] * len(args),
        out_specs=jax.tree.map(lambda _: VM, out_shape),
        scratch_shapes=scratch,
        compiler_params=params,
    )(*args)


def dft_table(n):
    k = np.arange(n)
    angle = 2.0 * np.pi / n * ((k[:, None] * k[None, :]) % n)
    full = np.concatenate([np.cos(angle), np.sin(angle)], axis=0).astype(np.float32)
    hi = full.astype(jnp.bfloat16)
    lo = (full - hi.astype(np.float32)).astype(jnp.bfloat16)
    return np.concatenate([hi, hi, lo], axis=1)


def body(links):
    n = EXTENT
    slices, local = links.shape[0], links.shape[-1]
    devices = lax.axis_size("space")
    plane = n * n
    q = local // n
    me = lax.axis_index("space")
    odd = me % 2
    shape = lambda *s: jax.ShapeDtypeStruct(s, f32)


    table = jnp.asarray(dft_table(n))
    site = jnp.arange(local, dtype=jnp.int32)
    coords = jnp.stack([site % n, (me * q + site // n - 1) % n])
    coords = jnp.broadcast_to(coords[:, None, :], (2, slices, local))
    across = jnp.transpose(links, (1, 2, 3, 4, 0, 5))
    alg = call(algebra_kernel, shape(3, 8, slices, local), [], across)
    mid = (n // 2) * n
    y_rim = from_behind(alg[1][..., local - plane :], "space", 1)
    z_below = from_behind(alg[2][..., local - LANES :], "space", 1)
    z_above = from_behind(
        jnp.where(odd == 1, alg[2][..., mid : mid + LANES], alg[2][..., :LANES]), "space", -1
    )
    head = -(-(local // 2) // (8 * n)) * 8 * n
    qh = head // n
    nsplit = 2
    count = n * nsplit // devices
    spread, theta = call(
        functools.partial(spread_kernel, n, head, nsplit),
        (shape(devices, q, LANES), shape(slices, LANES)),
        [pltpu.VMEM((LANES, head), f32), pltpu.VMEM((head, LANES), f32), pltpu.VMEM((head, LANES), f32)],
        alg, y_rim, z_below, z_above, coords, table,
    )
    planes = lax.all_to_all(spread, "space", split_axis=0, concat_axis=0, tiled=True)
    wave_np = (4.0 * np.sin(np.pi * np.arange(n) / n) ** 2).astype(np.float32)
    wave = jnp.broadcast_to(jnp.asarray(wave_np)[:, None], (n, LANES))
    slot = (np.arange(LANES) % HALF) // SEG
    kx = (me // nsplit) * count + jnp.minimum(jnp.asarray(slot), count - 1)
    wave_lane = jnp.asarray(wave_np)[kx][None, :]
    smoothed = call(
        functools.partial(plane_kernel, n),
        shape(plane, LANES),
        [pltpu.VMEM((plane, LANES), f32), pltpu.VMEM((plane, LANES), f32)],
        planes.reshape(plane, LANES), wave, wave_lane, table,
    )
    back = lax.all_to_all(
        smoothed.reshape(devices, q, LANES), "space", split_axis=0, concat_axis=0, tiled=True
    )
    smooth = call(
        functools.partial(gather_kernel, n, head, nsplit),
        shape(8, slices, local),
        [pltpu.VMEM((LANES, head), f32), pltpu.VMEM((head, LANES), f32), pltpu.VMEM((head, LANES), f32)],
        back, table,
    )
    above = from_behind(smooth[..., :plane], "space", -1)
    below = from_behind(
        jnp.where(odd == 1, smooth[..., mid : mid + LANES], smooth[..., plane : plane + LANES]), "space", 1
    )
    turned, deficit = call(
        functools.partial(link_kernel, n),
        (shape(3, 2, 3, 2, slices, local), shape(slices, LANES)),
        [pltpu.VMEM((18, slices, local + plane + LANES), f32)],
        across, smooth, above, below, coords,
    )
    new_links = jnp.transpose(turned, (4, 0, 1, 2, 3, 5))
    sums = call(
        functools.partial(sum_kernel, devices),
        shape(slices, LANES),
        [
            pltpu.VMEM((slices, LANES), f32),
            pltpu.VMEM((devices, slices, LANES), f32),
            pltpu.SemaphoreType.DMA((devices,)),
            pltpu.SemaphoreType.DMA((devices,)),
        ],
        theta, deficit,
        params=pltpu.CompilerParams(collective_id=1, has_side_effects=True),
    )
    total = sums[0, 1]
    times = lax.axis_size("tm")
    if times > 1:
        total = lax.psum(total, "tm")
    return (new_links, total / (slices * times * n**3), sums[:, 0] / n**3)


def solution(mesh):
    placed = (P("tm", None, None, None, None, "space"),)
    return jax.shard_map(
        body,
        mesh=mesh,
        in_specs=placed,
        out_specs=(P("tm", None, None, None, None, "space"), P(), P("tm")),
        check_vma=False,
    )
```

```python
import functools
import math

import jax
import jax.numpy as jnp
import numpy as np
from jax import lax
from jax.experimental import pallas as pl
from jax.experimental.pallas import tpu as pltpu
from jax.sharding import PartitionSpec as P

EXTENT = 48
LANES = 128
HALF = 64
SEG = 16

root_three = math.sqrt(3.0)
step_size = 0.08
top_momentum = 12.0

f32 = jnp.float32
bf16 = jnp.bfloat16
MESH = pl.DeviceIdType.MESH
VM = pl.BlockSpec(memory_space=pltpu.VMEM)
PARAMS = pltpu.CompilerParams(vmem_limit_bytes=60 * 1024 * 1024)


def cmul(p, q):
    return (p[0] * q[0] - p[1] * q[1], p[0] * q[1] + p[1] * q[0])


def cadd(p, q):
    return (p[0] + q[0], p[1] + q[1])


def csub(p, q):
    return (p[0] - q[0], p[1] - q[1])


def conj(p):
    return (p[0], -p[1])


def conj_mul(p, q):
    return (p[0] * q[0] + p[1] * q[1], p[0] * q[1] - p[1] * q[0])


def mul_conj(p, q):
    return (p[0] * q[0] + p[1] * q[1], p[1] * q[0] - p[0] * q[1])


def dot_row(row, col, mul):
    out = mul(row[0], col[0])
    for k in (1, 2):
        out = cadd(out, mul(row[k], col[k]))
    return out


def cross_conj(a, b):
    return [
        conj(csub(cmul(a[(k + 1) % 3], b[(k + 2) % 3]), cmul(a[(k + 2) % 3], b[(k + 1) % 3])))
        for k in range(3)
    ]


def algebra_of(u):
    return [
        u[0][1][1] + u[1][0][1],
        u[0][1][0] - u[1][0][0],
        u[0][0][1] - u[1][1][1],
        u[0][2][1] + u[2][0][1],
        u[0][2][0] - u[2][0][0],
        u[1][2][1] + u[2][1][1],
        u[1][2][0] - u[2][1][0],
        (u[0][0][1] + u[1][1][1] - 2.0 * u[2][2][1]) * (1.0 / root_three),
    ]


def rotation_of(s):
    h = 0.5 * step_size
    s = [v * h for v in s]
    third = s[7] * (1.0 / root_three)
    d0, d1, d2 = s[2] + third, third - s[2], -2.0 * third
    herm = [
        [(d0, None), (s[0], -s[1]), (s[3], -s[4])],
        [(s[0], s[1]), (d1, None), (s[5], -s[6])],
        [(s[3], s[4]), (s[5], s[6]), (d2, None)],
    ]

    def mul(p, q):
        if p[1] is None and q[1] is None:
            return (p[0] * q[0], jnp.zeros_like(p[0]))
        if p[1] is None:
            return (p[0] * q[0], p[0] * q[1])
        if q[1] is None:
            return (p[0] * q[0], p[1] * q[0])
        return cmul(p, q)

    rows = []
    for i in range(2):
        row = []
        for j in range(3):
            sq = dot_row(herm[i], [herm[k][j] for k in range(3)], mul)
            re, im = -0.5 * sq[0], -0.5 * sq[1]
            if herm[i][j][1] is not None:
                re = re - herm[i][j][1]
            else:
                re = re + 1.0
            row.append((re, im + herm[i][j][0]))
        rows.append(row)

    def unit(row):
        inv = lax.rsqrt(sum(p[0] * p[0] + p[1] * p[1] for p in row))
        return [(p[0] * inv, p[1] * inv) for p in row]

    one = unit(rows[0])
    corr = dot_row(one, rows[1], conj_mul)
    two = unit([csub(rows[1][k], cmul(corr, one[k])) for k in range(3)])
    return [one, two, cross_conj(one, two)]


def block(k):
    return pl.ds(pl.multiple_of(k * LANES, LANES), LANES)


def lane_ids(rows=8):
    return lax.broadcasted_iota(jnp.int32, (rows, LANES), 1)


def load_link(ref, d, sl):
    rows = [[(ref[d, r, c, 0, :, sl], ref[d, r, c, 1, :, sl]) for c in range(3)] for r in range(2)]
    return rows + [cross_conj(rows[0], rows[1])]


def algebra_kernel(links, out):
    def step(k, carry):
        sl = block(k)
        for d in range(3):
            for a, v in enumerate(algebra_of(load_link(links, d, sl))):
                out[d, a, :, sl] = v
        return carry

    lax.fori_loop(0, links.shape[-1] // LANES, step, 0)


def split3(x):
    hi = x.astype(bf16)
    lo = (x - hi.astype(f32)).astype(bf16)
    return jnp.concatenate([hi, lo, hi], axis=0)


def transform(table, parts, sign):
    n = parts[0].shape[0]
    both = jnp.dot(table, split3(jnp.concatenate(parts, axis=1)), preferred_element_type=f32)
    outs = []
    for i in range(len(parts)):
        mine = both[:, i * LANES : (i + 1) * LANES]
        swapped = pltpu.roll(mine[n:], HALF, 1)
        outs.append(mine[:n] + jnp.where(lane_ids(n) < HALF, sign, -sign) * swapped)
    return outs


def packed_rows(q, count):
    free = HALF // SEG - count
    moved = -(-q * free // (count + free)) // 8 * 8
    return q - moved if free == 1 else q


def pack_rows(full, count):
    q = full.shape[0]
    kept = packed_rows(q, count)
    step = q - kept
    if step == 0:
        return full
    seg = lax.rem(lane_ids(step), HALF) // SEG
    pieces = []
    for m in range(count):
        moved = pltpu.roll(full[kept:], (count - m) * SEG, 1)
        pieces.append(jnp.where(seg == count, moved, full[m * step : (m + 1) * step]))
    return jnp.concatenate(pieces + [full[count * step : kept]], axis=0)


def unpack_rows(block_in, q, count):
    kept = block_in.shape[0]
    step = q - kept
    if step == 0:
        return block_in
    seg = lax.rem(lane_ids(step), HALF) // SEG
    tail = jnp.zeros((step, LANES), f32)
    for m in range(count):
        moved = pltpu.roll(block_in[m * step : (m + 1) * step], LANES - (count - m) * SEG, 1)
        tail = jnp.where(seg == m, moved, tail)
    return jnp.concatenate([block_in, tail], axis=0)


def spread_kernel(extent, head, nsplit, q, alg, y_rim, z_below, z_above, coords, table, out, theta, mat, rows, freq):
    nb = alg.shape[-1] // LANES
    yb = y_rim.shape[-1] // LANES
    qh = head // extent
    hb = head // LANES
    lane = lane_ids()
    mat[...] = jnp.zeros_like(mat)

    def step(k, total):
        sl = block(k)
        before = block(jnp.maximum(k - 1, 0))
        after = block(jnp.minimum(k + 1, nb - 1))
        edge_x = coords[0, :, sl] == 0
        edge_z = coords[1, :, sl] == 0
        second = (k >= hb).astype(jnp.int32)
        dst = block(k - second * hb)
        for a in range(8):
            x, y, z = alg[0, a, :, sl], alg[1, a, :, sl], alg[2, a, :, sl]
            near = pltpu.roll(jnp.where(lane == LANES - 1, alg[0, a, :, before], x), 1, 1)
            far = pltpu.roll(jnp.where(lane < extent - 1, alg[0, a, :, after], x), LANES - extent + 1, 1)
            bx = jnp.where(edge_x, far, near)
            by = jnp.where(
                k < yb,
                y_rim[a, :, block(jnp.minimum(k, yb - 1))],
                alg[1, a, :, block(jnp.maximum(k - yb, 0))],
            )
            prev = jnp.where(k == 0, z_below[a], alg[2, a, :, before])
            near = pltpu.roll(jnp.where(lane >= LANES - extent, prev, z), extent, 1)
            far = pltpu.roll(jnp.where(k == 0, alg[2, a, :, block(yb)], z_above[a]), extent, 1)
            bz = jnp.where(edge_z, far, near)
            b = (bx - x) + (by - y) + (bz - z)
            total = total + b * b
            mat[pl.ds(pl.multiple_of((a % 2) * HALF + second * (HALF // 2) + (a // 2) * 8, 8), 8), dst] = b
        return total

    theta[...] = lax.fori_loop(0, nb, step, jnp.zeros((8, LANES), f32))
    for k in range(hb):
        rows[k * LANES : (k + 1) * LANES, :] = mat[:, k * LANES : (k + 1) * LANES].T

    def dft(i, carry):
        parts = [rows[pl.ds(pl.multiple_of((2 * i + e) * extent, 8), extent), :] for e in range(2)]
        for e, v in enumerate(transform(table[...], parts, 1.0)):
            freq[pl.ds(pl.multiple_of((2 * i + e) * extent, 8), extent), :] = v
        return carry

    lax.fori_loop(0, qh // 2, dft, 0, unroll=2)
    count = extent // (out.shape[0] // nsplit)
    seg = lax.rem(lane_ids(qh), HALF) // SEG

    def pack(j, carry):
        vals = [freq[pl.ds(j * count + m, qh, stride=extent), :] for m in range(count)]
        for c in range(nsplit):
            full = []
            for h in range(2):
                acc = jnp.zeros((qh, LANES), f32)
                for m in range(count):
                    moved = pltpu.roll(vals[m], ((m - (2 * h + c)) * SEG) % LANES, 1)
                    acc = jnp.where(seg == m, moved, acc)
                full.append(acc[: qh if h == 0 else q - qh])
            out[j * nsplit + c] = pack_rows(jnp.concatenate(full, axis=0), count)
        return carry

    lax.fori_loop(0, out.shape[0] // nsplit, pack, 0)


def plane_kernel(extent, nsplit, planes, wave, table, out, one, two):
    n = extent
    total = n * n
    devices, kept = planes.shape[0], planes.shape[1]
    q = total // devices
    count = n * nsplit // devices
    scale = top_momentum / float(n) ** 3

    def fill(s, carry):
        two[pl.ds(pl.multiple_of(s * q, 8), q), :] = unpack_rows(planes[s], q, count)
        return carry

    lax.fori_loop(0, devices, fill, 0)
    for y in range(n - 1):
        one[y * n : (y + 1) * n, :] = two[y * n + 1 : (y + 1) * n + 1, :]
    one[total - n : total - 1, :] = two[total - n + 1 : total, :]
    one[total - 1 : total, :] = two[0:1, :]
    slot = jnp.minimum(lax.rem(lane_ids(n), HALF) // SEG, count - 1)
    kx = lax.div(lax.axis_index("space"), nsplit) * count + slot
    chosen = lax.broadcasted_iota(jnp.int32, (n, LANES), 0) == kx
    wave_lane = jnp.sum(jnp.where(chosen, wave[...], 0.0), axis=0, keepdims=True)

    def rows_at(i):
        return pl.ds(pl.multiple_of(i * n, 8), n)

    def along_z(i, carry):
        parts = [one[rows_at(2 * i + e), :] for e in range(2)]
        for e, v in enumerate(transform(table[...], parts, 1.0)):
            two[rows_at(2 * i + e), :] = v
        return carry

    lax.fori_loop(0, n // 2, along_z, 0, unroll=2)

    def along_y(i, carry):
        parts = [two[pl.ds(2 * i + e, n, stride=n), :] for e in range(2)]
        vals = transform(table[...], parts, 1.0)
        done = []
        for e, v in enumerate(vals):
            p2 = wave[...] + (wave_lane + wave[pl.ds(2 * i + e, 1), :])
            zero = p2 == 0.0
            done.append(v * jnp.where(zero, 0.0, scale / jnp.where(zero, 1.0, p2)))
        for e, v in enumerate(transform(table[...], done, -1.0)):
            one[rows_at(2 * i + e), :] = v
        return carry

    lax.fori_loop(0, n // 2, along_y, 0, unroll=2)

    def back_z(i, carry):
        parts = [one[pl.ds(2 * i + e, n, stride=n), :] for e in range(2)]
        for e, v in enumerate(transform(table[...], parts, -1.0)):
            two[rows_at(2 * i + e), :] = v
        return carry

    lax.fori_loop(0, n // 2, back_z, 0, unroll=2)
    one[0:1, :] = two[total - 1 : total, :]
    for y in range(n - 1):
        one[y * n + 1 : (y + 1) * n + 1, :] = two[y * n : (y + 1) * n, :]
    one[total - n + 1 : total, :] = two[total - n : total - 1, :]

    def put(s, carry):
        out[s] = pack_rows(one[pl.ds(pl.multiple_of(s * q, 8), q), :], count)
        return carry

    lax.fori_loop(0, devices, put, 0)


def gather_kernel(extent, head, nsplit, planes, table, out, rows, freq):
    hb = head // LANES
    qh = head // extent
    nb = out.shape[-1] // LANES
    q = out.shape[-1] // extent
    rest = q - qh
    count = extent // (planes.shape[0] // nsplit)
    seg = lax.rem(lane_ids(rest), HALF) // SEG
    seg_tail = lax.rem(lane_ids(qh - rest), HALF) // SEG

    def unpack(j, carry):
        full = [unpack_rows(planes[j * nsplit + c], q, count) for c in range(nsplit)]
        for m in range(count):
            acc = jnp.zeros((rest, LANES), f32)
            tail = jnp.zeros((qh - rest, LANES), f32)
            for c in range(nsplit):
                for h in range(2):
                    s = 2 * h + c
                    shift = ((s - m) * SEG) % LANES
                    lo = h * qh
                    acc = jnp.where(seg == s, pltpu.roll(full[c][lo : lo + rest], shift, 1), acc)
                    if h == 0:
                        tail = jnp.where(
                            seg_tail == s, pltpu.roll(full[c][rest:qh], shift, 1), tail
                        )
            freq[pl.ds(j * count + m, qh, stride=extent), :] = jnp.concatenate([acc, tail], axis=0)
        return carry

    lax.fori_loop(0, planes.shape[0] // nsplit, unpack, 0)

    def dft(i, carry):
        parts = [freq[pl.ds(pl.multiple_of((2 * i + e) * extent, 8), extent), :] for e in range(2)]
        for e, v in enumerate(transform(table[...], parts, -1.0)):
            rows[pl.ds(pl.multiple_of((2 * i + e) * extent, 8), extent), :] = v
        return carry

    lax.fori_loop(0, qh // 2, dft, 0, unroll=2)
    for k in range(hb):
        turned = rows[k * LANES : (k + 1) * LANES, :].T
        for a in range(8):
            first = (a % 2) * HALF + (a // 2) * 8
            out[a, :, k * LANES : (k + 1) * LANES] = turned[first : first + 8]
            if hb + k < nb:
                second = first + HALF // 2
                out[a, :, (hb + k) * LANES : (hb + k + 1) * LANES] = turned[second : second + 8]


def link_kernel(extent, links, smooth, above, below, coords, out, deficit, rot):
    nb = smooth.shape[-1] // LANES
    yb = above.shape[-1] // LANES
    lane = lane_ids()

    def rotate(values, sl):
        g = rotation_of(values)
        for i in range(3):
            for j in range(3):
                for p in range(2):
                    rot[6 * i + 2 * j + p, :, sl] = g[i][j][p]

    def rotate_own(k, carry):
        rotate([smooth[a, :, block(k)] for a in range(8)], block(k))
        return carry

    def rotate_above(k, carry):
        rotate([above[a, :, block(k)] for a in range(8)], block(nb + k))
        return carry

    lax.fori_loop(0, nb, rotate_own, 0)
    lax.fori_loop(0, yb, rotate_above, 0)
    rotate([below[a] for a in range(8)], block(nb + yb))

    def step(k, total):
        sl = block(k)
        before = block(jnp.maximum(k - 1, 0))
        after = block(k + 1)
        wrap = block(jnp.where(k == yb, 0, nb + yb))
        edge_x = coords[0, :, sl] == extent - 1
        edge_z = coords[1, :, sl] == extent - 1

        def ahead_x(e):
            cur = rot[e, :, sl]
            near = pltpu.roll(jnp.where(lane == 0, rot[e, :, after], cur), LANES - 1, 1)
            far = pltpu.roll(jnp.where(lane >= LANES - extent + 1, rot[e, :, before], cur), extent - 1, 1)
            return jnp.where(edge_x, far, near)

        def ahead_y(e):
            return rot[e, :, block(k + yb)]

        def ahead_z(e):
            cur = rot[e, :, sl]
            near = pltpu.roll(jnp.where(lane < extent, rot[e, :, after], cur), LANES - extent, 1)
            far = pltpu.roll(rot[e, :, wrap], LANES - extent, 1)
            return jnp.where(edge_z, far, near)

        for d, ahead in enumerate((ahead_x, ahead_y, ahead_z)):
            u = load_link(links, d, sl)
            own = [[(rot[6 * i + 2 * j, :, sl], rot[6 * i + 2 * j + 1, :, sl]) for j in range(3)] for i in range(3)]
            left = [
                [dot_row(own[i], [u[k2][j] for k2 in range(3)], cmul) for j in range(3)]
                for i in range(3)
            ]
            for j in range(3):
                row = [(ahead(6 * j + 2 * c), ahead(6 * j + 2 * c + 1)) for c in range(3)]
                for i in range(2):
                    v = dot_row(left[i], row, mul_conj)
                    out[d, i, j, 0, :, sl] = v[0]
                    out[d, i, j, 1, :, sl] = v[1]
                    if i == j:
                        total = total + (1.0 - v[0])
                if j == 2:
                    total = total + (1.0 - dot_row(left[2], row, mul_conj)[0])
        return total

    deficit[...] = lax.fori_loop(0, nb, step, jnp.zeros((8, LANES), f32))


def greet(others):
    barrier = pltpu.get_barrier_semaphore()
    for other in others:
        pl.semaphore_signal(barrier, inc=1, device_id={"space": other}, device_id_type=MESH)
    return barrier


def exchange_kernel(n, blocks, out, send_sem, recv_sem):
    me = lax.axis_index("space")
    barrier = greet([lax.rem(me + i, n) for i in range(1, n)])
    out[me] = blocks[me]
    pl.semaphore_wait(barrier, n - 1)
    copies = []
    for i in range(1, n):
        other = lax.rem(me + i, n)
        copy = pltpu.make_async_remote_copy(
            src_ref=blocks.at[other],
            dst_ref=out.at[me],
            send_sem=send_sem.at[i],
            recv_sem=recv_sem.at[i],
            device_id={"space": other},
            device_id_type=MESH,
        )
        copy.start()
        copies.append(copy)
    for copy in copies:
        copy.wait()


def exchange(blocks, n, number):
    return call(
        functools.partial(exchange_kernel, n),
        jax.ShapeDtypeStruct(blocks.shape, f32),
        [pltpu.SemaphoreType.DMA((n,)), pltpu.SemaphoreType.DMA((n,))],
        blocks,
        params=pltpu.CompilerParams(collective_id=number, has_side_effects=True),
    )


def halo_kernel(n, moves, source, *refs):
    outs, (send_sem, recv_sem) = refs[:-2], refs[-2:]
    me = lax.axis_index("space")
    ahead, behind = lax.rem(me + 1, n), lax.rem(me + n - 1, n)
    barrier = greet([ahead, behind])
    pl.semaphore_wait(barrier, 2)
    odd = lax.rem(me, 2)
    copies = []
    for i, (direction, select) in enumerate(moves):
        copy = pltpu.make_async_remote_copy(
            src_ref=select(source, odd),
            dst_ref=outs[i],
            send_sem=send_sem.at[i],
            recv_sem=recv_sem.at[i],
            device_id={"space": ahead if direction > 0 else behind},
            device_id_type=MESH,
        )
        copy.start()
        copies.append(copy)
    for copy in copies:
        copy.wait()


def halos(source, n, moves, shapes, number):
    count = len(moves)
    return call(
        functools.partial(halo_kernel, n, moves),
        shapes,
        [pltpu.SemaphoreType.DMA((count,)), pltpu.SemaphoreType.DMA((count,))],
        source,
        params=pltpu.CompilerParams(collective_id=number, has_side_effects=True),
    )


def sum_kernel(n, scales, theta, deficit, out_theta, out_deficit, mine, held, send_sem, recv_sem):
    me = lax.axis_index("space")
    barrier = greet([lax.rem(me + i, n) for i in range(1, n)])
    slices = deficit.shape[0]
    lane = lane_ids(slices)
    t = jnp.sum(jnp.sum(theta[...], axis=1, keepdims=True), axis=0, keepdims=True)
    d = jnp.sum(deficit[...], axis=1, keepdims=True)
    own = lax.broadcasted_iota(jnp.int32, (slices, LANES), 0)
    mine[...] = jnp.where(lane == own, d, jnp.where(lane == slices, jnp.where(own == 0, t, 0.0), 0.0))
    pl.semaphore_wait(barrier, n - 1)
    copies = []
    for i in range(1, n):
        copy = pltpu.make_async_remote_copy(
            src_ref=mine,
            dst_ref=held.at[i],
            send_sem=send_sem.at[i],
            recv_sem=recv_sem.at[i],
            device_id={"space": lax.rem(me + i, n)},
            device_id_type=MESH,
        )
        copy.start()
        copies.append(copy)
    for copy in copies:
        copy.wait()
    total = mine[...]
    for i in range(1, n):
        total = total + held[i]
    row = jnp.sum(total, axis=0, keepdims=True)
    out_deficit[...] = row[:, :slices] * scales[1]
    out_theta[...] = row[:, slices : slices + 1] * scales[0]


def call(kernel, out_shape, scratch, *args, params=PARAMS):
    return pl.pallas_call(
        kernel,
        out_shape=out_shape,
        in_specs=[VM] * len(args),
        out_specs=jax.tree.map(lambda _: VM, out_shape),
        scratch_shapes=scratch,
        compiler_params=params,
    )(*args)


def dft_table(n):
    k = np.arange(n)
    angle = 2.0 * np.pi / n * ((k[:, None] * k[None, :]) % n)
    full = np.concatenate([np.cos(angle), np.sin(angle)], axis=0).astype(np.float32)
    hi = full.astype(jnp.bfloat16)
    lo = (full - hi.astype(np.float32)).astype(jnp.bfloat16)
    return np.concatenate([hi, hi, lo], axis=1)


def body(links):
    n = EXTENT
    slices, local = links.shape[0], links.shape[-1]
    devices = lax.axis_size("space")
    plane = n * n
    q = local // n
    me = lax.axis_index("space")
    shape = lambda *s: jax.ShapeDtypeStruct(s, f32)


    table = jnp.asarray(dft_table(n))
    site = jnp.arange(local, dtype=jnp.int32)
    coords = jnp.stack([site % n, (me * q + site // n - 1) % n])
    coords = jnp.broadcast_to(coords[:, None, :], (2, slices, local))
    across = jnp.transpose(links, (1, 2, 3, 4, 0, 5))
    alg = call(algebra_kernel, shape(3, 8, slices, local), [], across)
    mid = (n // 2) * n
    side = lambda start: pl.ds(pl.multiple_of(start, LANES), LANES)
    y_rim, z_below, z_above = halos(
        alg,
        devices,
        [
            (1, lambda r, odd: r.at[1, :, :, local - plane :]),
            (1, lambda r, odd: r.at[2, :, :, local - LANES :]),
            (-1, lambda r, odd: r.at[2, :, :, side(odd * mid)]),
        ],
        (shape(8, slices, plane), shape(8, slices, LANES), shape(8, slices, LANES)),
        2,
    )
    head = -(-(local // 2) // (8 * n)) * 8 * n
    qh = head // n
    nsplit = 2
    kept = packed_rows(q, n * nsplit // devices)
    spread, theta = call(
        functools.partial(spread_kernel, n, head, nsplit, q),
        (shape(devices, kept, LANES), shape(slices, LANES)),
        [pltpu.VMEM((LANES, head), f32), pltpu.VMEM((head, LANES), f32), pltpu.VMEM((head, LANES), f32)],
        alg, y_rim, z_below, z_above, coords, table,
    )
    planes = exchange(spread, devices, 3)
    wave_np = (4.0 * np.sin(np.pi * np.arange(n) / n) ** 2).astype(np.float32)
    wave = jnp.asarray(np.ascontiguousarray(np.broadcast_to(wave_np[:, None], (n, LANES))))
    smoothed = call(
        functools.partial(plane_kernel, n, nsplit),
        shape(devices, kept, LANES),
        [pltpu.VMEM((plane, LANES), f32), pltpu.VMEM((plane, LANES), f32)],
        planes, wave, table,
    )
    back = exchange(smoothed, devices, 4)
    smooth = call(
        functools.partial(gather_kernel, n, head, nsplit),
        shape(8, slices, local),
        [pltpu.VMEM((head, LANES), f32), pltpu.VMEM((head, LANES), f32)],
        back, table,
    )
    above, below = halos(
        smooth,
        devices,
        [
            (-1, lambda r, odd: r.at[:, :, :plane]),
            (1, lambda r, odd: r.at[:, :, side(plane - odd * (plane - mid))]),
        ],
        (shape(8, slices, plane), shape(8, slices, LANES)),
        5,
    )
    turned, deficit = call(
        functools.partial(link_kernel, n),
        (shape(3, 2, 3, 2, slices, local), shape(slices, LANES)),
        [pltpu.VMEM((18, slices, local + plane + LANES), f32)],
        across, smooth, above, below, coords,
    )
    new_links = jnp.transpose(turned, (4, 0, 1, 2, 3, 5))
    times = lax.axis_size("tm")
    scales = (1.0 / (slices * times * n**3), 1.0 / n**3)
    total, shares = call(
        functools.partial(sum_kernel, devices, scales),
        (shape(1, 1), shape(1, slices)),
        [
            pltpu.VMEM((slices, LANES), f32),
            pltpu.VMEM((devices, slices, LANES), f32),
            pltpu.SemaphoreType.DMA((devices,)),
            pltpu.SemaphoreType.DMA((devices,)),
        ],
        theta, deficit,
        params=pltpu.CompilerParams(collective_id=1, has_side_effects=True),
    )
    total = total.reshape(())
    if times > 1:
        total = lax.psum(total, "tm")
    return (new_links, total, shares.reshape(slices))


def solution(mesh):
    placed = (P("tm", None, None, None, None, "space"),)
    return jax.shard_map(
        body,
        mesh=mesh,
        in_specs=placed,
        out_specs=(P("tm", None, None, None, None, "space"), P(), P("tm")),
        check_vma=False,
    )
```

```python
import functools
import math

import jax
import jax.numpy as jnp
import numpy as np
from jax import lax
from jax.experimental import pallas as pl
from jax.experimental.pallas import tpu as pltpu
from jax.sharding import PartitionSpec as P

EXTENT = 48
LANES = 128
HALF = 64
SEG = 16

root_three = math.sqrt(3.0)
step_size = 0.08
top_momentum = 12.0

f32 = jnp.float32
bf16 = jnp.bfloat16
MESH = pl.DeviceIdType.MESH
VM = pl.BlockSpec(memory_space=pltpu.VMEM)
PARAMS = pltpu.CompilerParams(vmem_limit_bytes=60 * 1024 * 1024)


def cmul(p, q):
    return (p[0] * q[0] - p[1] * q[1], p[0] * q[1] + p[1] * q[0])


def cadd(p, q):
    return (p[0] + q[0], p[1] + q[1])


def csub(p, q):
    return (p[0] - q[0], p[1] - q[1])


def conj(p):
    return (p[0], -p[1])


def conj_mul(p, q):
    return (p[0] * q[0] + p[1] * q[1], p[0] * q[1] - p[1] * q[0])


def mul_conj(p, q):
    return (p[0] * q[0] + p[1] * q[1], p[1] * q[0] - p[0] * q[1])


def dot_row(row, col, mul):
    out = mul(row[0], col[0])
    for k in (1, 2):
        out = cadd(out, mul(row[k], col[k]))
    return out


def cross_conj(a, b):
    return [
        conj(csub(cmul(a[(k + 1) % 3], b[(k + 2) % 3]), cmul(a[(k + 2) % 3], b[(k + 1) % 3])))
        for k in range(3)
    ]


def algebra_of(u):
    return [
        u[0][1][1] + u[1][0][1],
        u[0][1][0] - u[1][0][0],
        u[0][0][1] - u[1][1][1],
        u[0][2][1] + u[2][0][1],
        u[0][2][0] - u[2][0][0],
        u[1][2][1] + u[2][1][1],
        u[1][2][0] - u[2][1][0],
        (u[0][0][1] + u[1][1][1] - 2.0 * u[2][2][1]) * (1.0 / root_three),
    ]


def rotation_of(s):
    h = 0.5 * step_size
    s = [v * h for v in s]
    third = s[7] * (1.0 / root_three)
    d0, d1, d2 = s[2] + third, third - s[2], -2.0 * third
    herm = [
        [(d0, None), (s[0], -s[1]), (s[3], -s[4])],
        [(s[0], s[1]), (d1, None), (s[5], -s[6])],
        [(s[3], s[4]), (s[5], s[6]), (d2, None)],
    ]

    def mul(p, q):
        if p[1] is None and q[1] is None:
            return (p[0] * q[0], jnp.zeros_like(p[0]))
        if p[1] is None:
            return (p[0] * q[0], p[0] * q[1])
        if q[1] is None:
            return (p[0] * q[0], p[1] * q[0])
        return cmul(p, q)

    rows = []
    for i in range(2):
        row = []
        for j in range(3):
            sq = dot_row(herm[i], [herm[k][j] for k in range(3)], mul)
            re, im = -0.5 * sq[0], -0.5 * sq[1]
            if herm[i][j][1] is not None:
                re = re - herm[i][j][1]
            else:
                re = re + 1.0
            row.append((re, im + herm[i][j][0]))
        rows.append(row)

    def unit(row):
        inv = lax.rsqrt(sum(p[0] * p[0] + p[1] * p[1] for p in row))
        return [(p[0] * inv, p[1] * inv) for p in row]

    one = unit(rows[0])
    corr = dot_row(one, rows[1], conj_mul)
    two = unit([csub(rows[1][k], cmul(corr, one[k])) for k in range(3)])
    return [one, two, cross_conj(one, two)]


def block(k):
    return pl.ds(pl.multiple_of(k * LANES, LANES), LANES)


def lane_ids(rows=8):
    return lax.broadcasted_iota(jnp.int32, (rows, LANES), 1)


def load_link(ref, d, sl):
    rows = [[(ref[d, r, c, 0, :, sl], ref[d, r, c, 1, :, sl]) for c in range(3)] for r in range(2)]
    return rows + [cross_conj(rows[0], rows[1])]


def algebra_kernel(links, out):
    def step(k, carry):
        sl = block(k)
        for d in range(3):
            for a, v in enumerate(algebra_of(load_link(links, d, sl))):
                out[d, a, :, sl] = v
        return carry

    lax.fori_loop(0, links.shape[-1] // LANES, step, 0)


def split3(x):
    hi = x.astype(bf16)
    lo = (x - hi.astype(f32)).astype(bf16)
    return jnp.concatenate([hi, lo, hi], axis=0)


def transform(table, parts, sign):
    n = parts[0].shape[0]
    both = jnp.dot(table, split3(jnp.concatenate(parts, axis=1)), preferred_element_type=f32)
    outs = []
    for i in range(len(parts)):
        mine = both[:, i * LANES : (i + 1) * LANES]
        swapped = pltpu.roll(mine[n:], HALF, 1)
        outs.append(mine[:n] + jnp.where(lane_ids(n) < HALF, sign, -sign) * swapped)
    return outs


def packed_rows(q, count):
    free = HALF // SEG - count
    moved = -(-q * free // (count + free)) // 8 * 8
    return q - moved if free == 1 else q


def pack_rows(full, count):
    q = full.shape[0]
    kept = packed_rows(q, count)
    step = q - kept
    if step == 0:
        return full
    seg = lax.rem(lane_ids(step), HALF) // SEG
    pieces = []
    for m in range(count):
        moved = pltpu.roll(full[kept:], (count - m) * SEG, 1)
        pieces.append(jnp.where(seg == count, moved, full[m * step : (m + 1) * step]))
    return jnp.concatenate(pieces + [full[count * step : kept]], axis=0)


def unpack_rows(block_in, q, count):
    kept = block_in.shape[0]
    step = q - kept
    if step == 0:
        return block_in
    seg = lax.rem(lane_ids(step), HALF) // SEG
    tail = jnp.zeros((step, LANES), f32)
    for m in range(count):
        moved = pltpu.roll(block_in[m * step : (m + 1) * step], LANES - (count - m) * SEG, 1)
        tail = jnp.where(seg == m, moved, tail)
    return jnp.concatenate([block_in, tail], axis=0)


def spread_kernel(extent, head, nsplit, q, alg, y_rim, z_below, z_above, coords, table, out, theta, mat, rows, freq):
    nb = alg.shape[-1] // LANES
    yb = y_rim.shape[-1] // LANES
    qh = head // extent
    hb = head // LANES
    lane = lane_ids()
    mat[...] = jnp.zeros_like(mat)

    def step(k, total):
        sl = block(k)
        before = block(jnp.maximum(k - 1, 0))
        after = block(jnp.minimum(k + 1, nb - 1))
        edge_x = coords[0, :, sl] == 0
        edge_z = coords[1, :, sl] == 0
        second = (k >= hb).astype(jnp.int32)
        dst = block(k - second * hb)
        for a in range(8):
            x, y, z = alg[0, a, :, sl], alg[1, a, :, sl], alg[2, a, :, sl]
            near = pltpu.roll(jnp.where(lane == LANES - 1, alg[0, a, :, before], x), 1, 1)
            far = pltpu.roll(jnp.where(lane < extent - 1, alg[0, a, :, after], x), LANES - extent + 1, 1)
            bx = jnp.where(edge_x, far, near)
            by = jnp.where(
                k < yb,
                y_rim[a, :, block(jnp.minimum(k, yb - 1))],
                alg[1, a, :, block(jnp.maximum(k - yb, 0))],
            )
            prev = jnp.where(k == 0, z_below[a], alg[2, a, :, before])
            near = pltpu.roll(jnp.where(lane >= LANES - extent, prev, z), extent, 1)
            far = pltpu.roll(jnp.where(k == 0, alg[2, a, :, block(yb)], z_above[a]), extent, 1)
            bz = jnp.where(edge_z, far, near)
            b = (bx - x) + (by - y) + (bz - z)
            total = total + b * b
            mat[pl.ds(pl.multiple_of((a % 2) * HALF + second * (HALF // 2) + (a // 2) * 8, 8), 8), dst] = b
        return total

    theta[...] = lax.fori_loop(0, nb, step, jnp.zeros((8, LANES), f32))
    for k in range(hb):
        rows[k * LANES : (k + 1) * LANES, :] = mat[:, k * LANES : (k + 1) * LANES].T

    def dft(i, carry):
        parts = [rows[pl.ds(pl.multiple_of((2 * i + e) * extent, 8), extent), :] for e in range(2)]
        for e, v in enumerate(transform(table[...], parts, 1.0)):
            freq[pl.ds(pl.multiple_of((2 * i + e) * extent, 8), extent), :] = v
        return carry

    lax.fori_loop(0, qh // 2, dft, 0, unroll=4)
    count = extent // (out.shape[0] // nsplit)
    seg = lax.rem(lane_ids(qh), HALF) // SEG

    def pack(j, carry):
        vals = [freq[pl.ds(j * count + m, qh, stride=extent), :] for m in range(count)]
        for c in range(nsplit):
            full = []
            for h in range(2):
                acc = jnp.zeros((qh, LANES), f32)
                for m in range(count):
                    moved = pltpu.roll(vals[m], ((m - (2 * h + c)) * SEG) % LANES, 1)
                    acc = jnp.where(seg == m, moved, acc)
                full.append(acc[: qh if h == 0 else q - qh])
            out[j * nsplit + c] = pack_rows(jnp.concatenate(full, axis=0), count)
        return carry

    lax.fori_loop(0, out.shape[0] // nsplit, pack, 0, unroll=2)


def plane_kernel(extent, nsplit, planes, wave, table, out, one, two):
    n = extent
    total = n * n
    devices, kept = planes.shape[0], planes.shape[1]
    q = total // devices
    count = n * nsplit // devices
    scale = top_momentum / float(n) ** 3

    for s in range(devices):
        rows = unpack_rows(planes[s], q, count)
        if s == 0:
            one[0 : q - 1, :] = rows[1:]
            one[total - 1 : total, :] = rows[:1]
        else:
            one[s * q - 1 : (s + 1) * q - 1, :] = rows
    slot = jnp.minimum(lax.rem(lane_ids(n), HALF) // SEG, count - 1)
    kx = lax.div(lax.axis_index("space"), nsplit) * count + slot
    chosen = lax.broadcasted_iota(jnp.int32, (n, LANES), 0) == kx
    wave_lane = jnp.sum(jnp.where(chosen, wave[...], 0.0), axis=0, keepdims=True)

    def rows_at(i):
        return pl.ds(pl.multiple_of(i * n, 8), n)

    def along_z(i, carry):
        parts = [one[rows_at(2 * i + e), :] for e in range(2)]
        for e, v in enumerate(transform(table[...], parts, 1.0)):
            two[rows_at(2 * i + e), :] = v
        return carry

    lax.fori_loop(0, n // 2, along_z, 0, unroll=4)

    def along_y(i, carry):
        parts = [two[pl.ds(2 * i + e, n, stride=n), :] for e in range(2)]
        vals = transform(table[...], parts, 1.0)
        done = []
        for e, v in enumerate(vals):
            p2 = wave[...] + (wave_lane + wave[pl.ds(2 * i + e, 1), :])
            zero = p2 == 0.0
            done.append(v * jnp.where(zero, 0.0, scale / jnp.where(zero, 1.0, p2)))
        for e, v in enumerate(transform(table[...], done, -1.0)):
            one[rows_at(2 * i + e), :] = v
        return carry

    lax.fori_loop(0, n // 2, along_y, 0, unroll=4)

    def back_z(i, carry):
        parts = [one[pl.ds(2 * i + e, n, stride=n), :] for e in range(2)]
        for e, v in enumerate(transform(table[...], parts, -1.0)):
            two[rows_at(2 * i + e), :] = v
        return carry

    lax.fori_loop(0, n // 2, back_z, 0, unroll=4)
    for s in range(devices):
        if s == 0:
            rows = jnp.concatenate([two[total - 1 : total, :], two[0 : q - 1, :]], axis=0)
        else:
            rows = two[s * q - 1 : (s + 1) * q - 1, :]
        out[s] = pack_rows(rows, count)


def gather_kernel(extent, head, nsplit, planes, table, out, rows, freq):
    hb = head // LANES
    qh = head // extent
    nb = out.shape[-1] // LANES
    q = out.shape[-1] // extent
    rest = q - qh
    count = extent // (planes.shape[0] // nsplit)
    seg = lax.rem(lane_ids(rest), HALF) // SEG
    seg_tail = lax.rem(lane_ids(qh - rest), HALF) // SEG

    def unpack(j, carry):
        full = [unpack_rows(planes[j * nsplit + c], q, count) for c in range(nsplit)]
        for m in range(count):
            acc = jnp.zeros((rest, LANES), f32)
            tail = jnp.zeros((qh - rest, LANES), f32)
            for c in range(nsplit):
                for h in range(2):
                    s = 2 * h + c
                    shift = ((s - m) * SEG) % LANES
                    lo = h * qh
                    acc = jnp.where(seg == s, pltpu.roll(full[c][lo : lo + rest], shift, 1), acc)
                    if h == 0:
                        tail = jnp.where(
                            seg_tail == s, pltpu.roll(full[c][rest:qh], shift, 1), tail
                        )
            freq[pl.ds(j * count + m, qh, stride=extent), :] = jnp.concatenate([acc, tail], axis=0)
        return carry

    lax.fori_loop(0, planes.shape[0] // nsplit, unpack, 0, unroll=2)

    def dft(i, carry):
        parts = [freq[pl.ds(pl.multiple_of((2 * i + e) * extent, 8), extent), :] for e in range(2)]
        for e, v in enumerate(transform(table[...], parts, -1.0)):
            rows[pl.ds(pl.multiple_of((2 * i + e) * extent, 8), extent), :] = v
        return carry

    lax.fori_loop(0, qh // 2, dft, 0, unroll=4)
    for k in range(hb):
        turned = rows[k * LANES : (k + 1) * LANES, :].T
        for a in range(8):
            first = (a % 2) * HALF + (a // 2) * 8
            out[a, :, k * LANES : (k + 1) * LANES] = turned[first : first + 8]
            if hb + k < nb:
                second = first + HALF // 2
                out[a, :, (hb + k) * LANES : (hb + k + 1) * LANES] = turned[second : second + 8]


def link_kernel(extent, links, smooth, above, below, coords, out, deficit, rot):
    nb = smooth.shape[-1] // LANES
    yb = above.shape[-1] // LANES
    lane = lane_ids()

    def rotate(values, sl):
        g = rotation_of(values)
        for i in range(3):
            for j in range(3):
                for p in range(2):
                    rot[6 * i + 2 * j + p, :, sl] = g[i][j][p]

    def rotate_own(k, carry):
        rotate([smooth[a, :, block(k)] for a in range(8)], block(k))
        return carry

    def rotate_above(k, carry):
        rotate([above[a, :, block(k)] for a in range(8)], block(nb + k))
        return carry

    lax.fori_loop(0, nb, rotate_own, 0)
    lax.fori_loop(0, yb, rotate_above, 0)
    rotate([below[a] for a in range(8)], block(nb + yb))

    def step(k, total):
        sl = block(k)
        before = block(jnp.maximum(k - 1, 0))
        after = block(k + 1)
        wrap = block(jnp.where(k == yb, 0, nb + yb))
        edge_x = coords[0, :, sl] == extent - 1
        edge_z = coords[1, :, sl] == extent - 1

        def ahead_x(e):
            cur = rot[e, :, sl]
            near = pltpu.roll(jnp.where(lane == 0, rot[e, :, after], cur), LANES - 1, 1)
            far = pltpu.roll(jnp.where(lane >= LANES - extent + 1, rot[e, :, before], cur), extent - 1, 1)
            return jnp.where(edge_x, far, near)

        def ahead_y(e):
            return rot[e, :, block(k + yb)]

        def ahead_z(e):
            cur = rot[e, :, sl]
            near = pltpu.roll(jnp.where(lane < extent, rot[e, :, after], cur), LANES - extent, 1)
            far = pltpu.roll(rot[e, :, wrap], LANES - extent, 1)
            return jnp.where(edge_z, far, near)

        for d, ahead in enumerate((ahead_x, ahead_y, ahead_z)):
            u = load_link(links, d, sl)
            own = [[(rot[6 * i + 2 * j, :, sl], rot[6 * i + 2 * j + 1, :, sl]) for j in range(3)] for i in range(3)]
            left = [
                [dot_row(own[i], [u[k2][j] for k2 in range(3)], cmul) for j in range(3)]
                for i in range(3)
            ]
            for j in range(3):
                row = [(ahead(6 * j + 2 * c), ahead(6 * j + 2 * c + 1)) for c in range(3)]
                for i in range(2):
                    v = dot_row(left[i], row, mul_conj)
                    out[d, i, j, 0, :, sl] = v[0]
                    out[d, i, j, 1, :, sl] = v[1]
                    if i == j:
                        total = total + (1.0 - v[0])
                if j == 2:
                    total = total + (1.0 - dot_row(left[2], row, mul_conj)[0])
        return total

    deficit[...] = lax.fori_loop(0, nb, step, jnp.zeros((8, LANES), f32))


def greet(others):
    barrier = pltpu.get_barrier_semaphore()
    for other in others:
        pl.semaphore_signal(barrier, inc=1, device_id={"space": other}, device_id_type=MESH)
    return barrier


def exchange_kernel(n, blocks, out, send_sem, recv_sem):
    me = lax.axis_index("space")

    def partner(i):
        if n & (n - 1):
            return lax.rem(me + i, n)
        other = me
        for b in range(n.bit_length() - 1):
            if i >> b & 1:
                other = other + (1 << b) * (1 - 2 * lax.rem(lax.div(me, 1 << b), 2))
        return other

    barrier = greet([partner(i) for i in range(1, n)])
    out[me] = blocks[me]
    pl.semaphore_wait(barrier, n - 1)
    copies = []
    for i in reversed(range(1, n)):
        other = partner(i)
        copy = pltpu.make_async_remote_copy(
            src_ref=blocks.at[other],
            dst_ref=out.at[me],
            send_sem=send_sem.at[i],
            recv_sem=recv_sem.at[i],
            device_id={"space": other},
            device_id_type=MESH,
        )
        copy.start()
        copies.append(copy)
    for copy in copies:
        copy.wait()


def exchange(blocks, n, number):
    return call(
        functools.partial(exchange_kernel, n),
        jax.ShapeDtypeStruct(blocks.shape, f32),
        [pltpu.SemaphoreType.DMA((n,)), pltpu.SemaphoreType.DMA((n,))],
        blocks,
        params=pltpu.CompilerParams(collective_id=number, has_side_effects=True),
    )


def halo_kernel(n, moves, source, *refs):
    outs, (send_sem, recv_sem) = refs[:-2], refs[-2:]
    me = lax.axis_index("space")
    ahead, behind = lax.rem(me + 1, n), lax.rem(me + n - 1, n)
    barrier = greet([ahead, behind])
    pl.semaphore_wait(barrier, 2)
    odd = lax.rem(me, 2)
    copies = []
    for i, (direction, select) in enumerate(moves):
        copy = pltpu.make_async_remote_copy(
            src_ref=select(source, odd),
            dst_ref=outs[i],
            send_sem=send_sem.at[i],
            recv_sem=recv_sem.at[i],
            device_id={"space": ahead if direction > 0 else behind},
            device_id_type=MESH,
        )
        copy.start()
        copies.append(copy)
    for copy in copies:
        copy.wait()


def halos(source, n, moves, shapes, number):
    count = len(moves)
    return call(
        functools.partial(halo_kernel, n, moves),
        shapes,
        [pltpu.SemaphoreType.DMA((count,)), pltpu.SemaphoreType.DMA((count,))],
        source,
        params=pltpu.CompilerParams(collective_id=number, has_side_effects=True),
    )


def sum_kernel(n, scales, theta, deficit, out_theta, out_deficit, mine, held, send_sem, recv_sem):
    me = lax.axis_index("space")
    barrier = greet([lax.rem(me + i, n) for i in range(1, n)])
    slices = deficit.shape[0]
    lane = lane_ids(slices)
    t = jnp.sum(jnp.sum(theta[...], axis=1, keepdims=True), axis=0, keepdims=True)
    d = jnp.sum(deficit[...], axis=1, keepdims=True)
    own = lax.broadcasted_iota(jnp.int32, (slices, LANES), 0)
    mine[...] = jnp.where(lane == own, d, jnp.where(lane == slices, jnp.where(own == 0, t, 0.0), 0.0))
    pl.semaphore_wait(barrier, n - 1)
    copies = []
    for i in range(1, n):
        copy = pltpu.make_async_remote_copy(
            src_ref=mine,
            dst_ref=held.at[i],
            send_sem=send_sem.at[i],
            recv_sem=recv_sem.at[i],
            device_id={"space": lax.rem(me + i, n)},
            device_id_type=MESH,
        )
        copy.start()
        copies.append(copy)
    for copy in copies:
        copy.wait()
    total = mine[...]
    for i in range(1, n):
        total = total + held[i]
    row = jnp.sum(total, axis=0, keepdims=True)
    out_deficit[...] = row[:, :slices] * scales[1]
    out_theta[...] = row[:, slices : slices + 1] * scales[0]


def call(kernel, out_shape, scratch, *args, params=PARAMS):
    return pl.pallas_call(
        kernel,
        out_shape=out_shape,
        in_specs=[VM] * len(args),
        out_specs=jax.tree.map(lambda _: VM, out_shape),
        scratch_shapes=scratch,
        compiler_params=params,
    )(*args)


def dft_table(n):
    k = np.arange(n)
    angle = 2.0 * np.pi / n * ((k[:, None] * k[None, :]) % n)
    full = np.concatenate([np.cos(angle), np.sin(angle)], axis=0).astype(np.float32)
    hi = full.astype(jnp.bfloat16)
    lo = (full - hi.astype(np.float32)).astype(jnp.bfloat16)
    return np.concatenate([hi, hi, lo], axis=1)


def body(links):
    n = EXTENT
    slices, local = links.shape[0], links.shape[-1]
    devices = lax.axis_size("space")
    plane = n * n
    q = local // n
    me = lax.axis_index("space")
    shape = lambda *s: jax.ShapeDtypeStruct(s, f32)


    table = jnp.asarray(dft_table(n))
    site = jnp.arange(local, dtype=jnp.int32)
    coords = jnp.stack([site % n, (me * q + site // n - 1) % n])
    coords = jnp.broadcast_to(coords[:, None, :], (2, slices, local))
    across = jnp.transpose(links, (1, 2, 3, 4, 0, 5))
    alg = call(algebra_kernel, shape(3, 8, slices, local), [], across)
    mid = (n // 2) * n
    side = lambda start: pl.ds(pl.multiple_of(start, LANES), LANES)
    y_rim, z_below, z_above = halos(
        alg,
        devices,
        [
            (1, lambda r, odd: r.at[1, :, :, local - plane :]),
            (1, lambda r, odd: r.at[2, :, :, local - LANES :]),
            (-1, lambda r, odd: r.at[2, :, :, side(odd * mid)]),
        ],
        (shape(8, slices, plane), shape(8, slices, LANES), shape(8, slices, LANES)),
        2,
    )
    head = -(-(local // 2) // (8 * n)) * 8 * n
    qh = head // n
    nsplit = 2
    kept = packed_rows(q, n * nsplit // devices)
    spread, theta = call(
        functools.partial(spread_kernel, n, head, nsplit, q),
        (shape(devices, kept, LANES), shape(slices, LANES)),
        [pltpu.VMEM((LANES, head), f32), pltpu.VMEM((head, LANES), f32), pltpu.VMEM((head, LANES), f32)],
        alg, y_rim, z_below, z_above, coords, table,
    )
    planes = exchange(spread, devices, 3)
    wave_np = (4.0 * np.sin(np.pi * np.arange(n) / n) ** 2).astype(np.float32)
    wave = jnp.asarray(np.ascontiguousarray(np.broadcast_to(wave_np[:, None], (n, LANES))))
    smoothed = call(
        functools.partial(plane_kernel, n, nsplit),
        shape(devices, kept, LANES),
        [pltpu.VMEM((plane, LANES), f32), pltpu.VMEM((plane, LANES), f32)],
        planes, wave, table,
    )
    back = exchange(smoothed, devices, 4)
    smooth = call(
        functools.partial(gather_kernel, n, head, nsplit),
        shape(8, slices, local),
        [pltpu.VMEM((head, LANES), f32), pltpu.VMEM((head, LANES), f32)],
        back, table,
    )
    above, below = halos(
        smooth,
        devices,
        [
            (-1, lambda r, odd: r.at[:, :, :plane]),
            (1, lambda r, odd: r.at[:, :, side(plane - odd * (plane - mid))]),
        ],
        (shape(8, slices, plane), shape(8, slices, LANES)),
        5,
    )
    turned, deficit = call(
        functools.partial(link_kernel, n),
        (shape(3, 2, 3, 2, slices, local), shape(slices, LANES)),
        [pltpu.VMEM((18, slices, local + plane + LANES), f32)],
        across, smooth, above, below, coords,
    )
    new_links = jnp.transpose(turned, (4, 0, 1, 2, 3, 5))
    times = lax.axis_size("tm")
    scales = (1.0 / (slices * times * n**3), 1.0 / n**3)
    total, shares = call(
        functools.partial(sum_kernel, devices, scales),
        (shape(1, 1), shape(1, slices)),
        [
            pltpu.VMEM((slices, LANES), f32),
            pltpu.VMEM((devices, slices, LANES), f32),
            pltpu.SemaphoreType.DMA((devices,)),
            pltpu.SemaphoreType.DMA((devices,)),
        ],
        theta, deficit,
        params=pltpu.CompilerParams(collective_id=1, has_side_effects=True),
    )
    total = total.reshape(())
    if times > 1:
        total = lax.psum(total, "tm")
    return (new_links, total, shares.reshape(slices))


def solution(mesh):
    placed = (P("tm", None, None, None, None, "space"),)
    return jax.shard_map(
        body,
        mesh=mesh,
        in_specs=placed,
        out_specs=(P("tm", None, None, None, None, "space"), P(), P("tm")),
        check_vma=False,
    )
```
